128 devices in a mesh: lev: 4 (over y), col: 32 (over z, x, core).
Axes of the slice: x: 4, y: 4, z: 4, core: 2. Of those that a mesh axis runs over, the one named last changes fastest.
Arguments:
- control_field: float32 [96, 16, 768, 128], P('lev', None, 'col'), may hold values from -24 to 24
- decay_rate: float32 [96, 768, 128], P('lev', 'col'), may hold values from 0.5 to 0.999
- diffusivity: float32 [768, 128], P('col'), may hold values from 0.08 to 0.24
Outputs:
- localized: float32 [96, 16, 768, 128], P('lev', None, 'col')
The draws below stay inside these ranges and needn't reach their ends.
All inputs are finite; a program needn't handle non-finite values.
Results may differ from the reference program's by a relative error of at most 0.00002.
Values sent between devices are 32-bit elements; how exact they have to be, the bound alone decides.
A program may use at most 64 MiB of HBM per device.

```python
import math
import jax
import jax.numpy as jnp
from jax import lax

MEMBERS = 16
LATITUDE_ROWS = 128
SMOOTH = 4
WINDOW_LEVELS = 96
WINDOW_LONGITUDES = 768


def draw_decay_rate(key, part):
    key_scale = jax.random.fold_in(key, 11)
    key_rough = jax.random.fold_in(key, 12)
    spike_key = jax.random.fold_in(key, 13)
    depth_key = jax.random.fold_in(key, 14)
    low_scale = 4.0
    high_scale = 4.0 * WINDOW_LEVELS
    column_scale = jnp.exp(jax.random.uniform(key_scale, (1, WINDOW_LONGITUDES, LATITUDE_ROWS), jnp.float32, jnp.log(low_scale), jnp.log(high_scale)))
    roughness = jax.random.uniform(key_rough, (WINDOW_LEVELS, WINDOW_LONGITUDES, LATITUDE_ROWS), jnp.float32, 0.5, 1.5)
    decay_rates = jnp.exp(-1.0 / (column_scale * roughness))
    spike_levels = jax.random.randint(spike_key, (3,), 0, WINDOW_LEVELS)
    level_numbers = jnp.arange(WINDOW_LEVELS, dtype=jnp.int32)
    spike_present = jnp.any(level_numbers[:, None] == spike_levels[None, :], axis=1)
    spike_depth = jax.random.uniform(depth_key, (1, WINDOW_LONGITUDES, LATITUDE_ROWS), jnp.float32, 0.5, 0.8)
    decay_rates = jnp.where(spike_present[:, None, None], decay_rates * spike_depth, decay_rates)
    return jnp.clip(decay_rates, 0.5, 0.999).astype(jnp.float32)


def block_scale(rng, extent, cuts, low, high):
    gain, own = 1.0, jax.random.fold_in(rng, 6)
    for axis_at, parts in cuts:
        draws = jnp.exp(jax.random.uniform(jax.random.fold_in(own, axis_at), (parts,), jnp.float32, low / len(cuts), high / len(cuts)))
        gain = gain * jnp.repeat(draws, extent[axis_at] // parts).reshape([-1 if axis == axis_at else 1 for axis in range(len(extent))])
    return gain


def scatter_about(rng, extent, spread, most, split=(), held_as=jnp.bfloat16):
    entries = jax.random.normal(rng, extent, jnp.float32) * spread
    if len(split) > 0:
        entries = block_scale(rng, extent, split, -0.22, 0.18) * entries
    return jnp.clip(entries, min=-most, max=most).astype(held_as)


def setup_inputs(seed: int = 0) -> dict:
    seeds = jax.random.split(jax.random.key(seed), 4)
    control_field = scatter_about(seeds[0], (WINDOW_LEVELS, MEMBERS, WINDOW_LONGITUDES, LATITUDE_ROWS), 4.0, 24.0, ((0, 4), (2, 32)), jnp.float32)
    decay_rate = draw_decay_rate(jax.random.fold_in(seeds[3], 71), 0)
    diffusivity = jnp.clip(jnp.exp(math.log(0.24) - 1.0986123 * jax.random.uniform(seeds[2], (WINDOW_LONGITUDES, LATITUDE_ROWS), jnp.float32) ** block_scale(seeds[2], (WINDOW_LONGITUDES, LATITUDE_ROWS), ((0, 32),), -0.2, 0.2)), 0.08, 0.24)
    return dict(control_field=control_field, decay_rate=decay_rate, diffusivity=diffusivity)


def recursion(decay_rates, field, backward):
    def advance(state, inputs):
        weight, values = inputs
        state = weight * state + (1.0 - weight) * values
        return state, state

    start = jnp.zeros(field.shape[1:], jnp.float32)
    unused, swept = lax.scan(advance, start, (decay_rates[:, None], field), reverse=backward)
    return swept


def lat_sum(field):
    padded = jnp.pad(field, ((0, 0), (0, 0), (0, 0), (1, 1)))
    return padded[..., 2:] + padded[..., :-2]


def lon_sum(field):
    padded = jnp.pad(field, ((0, 0), (0, 0), (1, 1), (0, 0)))
    return padded[:, :, 2:] + padded[:, :, :-2]


def reference(control_field, decay_rate, diffusivity):
    filtered = control_field
    for repeat in range(2):
        filtered = recursion(decay_rate, filtered, False)
        filtered = recursion(decay_rate, filtered, True)
    current = filtered
    for position in range(SMOOTH):
        current = current + diffusivity[None, None] * (lon_sum(current) + lat_sum(current) - 4.0 * current)
    return current
```

```python
import functools

import jax
import jax.numpy as jnp
from jax import lax
from jax.experimental import pallas as pl
from jax.experimental.pallas import tpu as pltpu
from jax.sharding import PartitionSpec as P

MESH = pl.DeviceIdType.MESH
SMOOTH = 4
PAIR = 2
LAG = 6
HALO_LAG = 6


def kernel(n_lev, n_col, x_hbm, w_hbm, kap_ref, y_ref, wv, bv, G, C, E, rin, rout, qin, qout, hs, hin, U, T, ks, kin, kw,
           kc, wsem, xsem, rsend, rrecv, qsend, qrecv, hsend, hrecv, ksend, krecv):
    levels, members, lons, lats = x_hbm.shape
    d, c = lax.axis_index("lev"), lax.axis_index("col")
    has_low, has_high = d > 0, d < n_lev - 1
    has_left, has_right = c > 0, c < n_col - 1
    middle = jnp.logical_and(has_low, has_high)

    barrier = pltpu.get_barrier_semaphore()
    for there, where in ((has_low, {"lev": d - 1}), (has_high, {"lev": d + 1}), (has_left, {"col": c - 1}), (has_right, {"col": c + 1})):
        @pl.when(there)
        def _():
            pl.semaphore_signal(barrier, inc=1, device_id=where, device_id_type=MESH)

    w_copy = pltpu.make_async_copy(w_hbm, wv, wsem)
    w_copy.start()

    def x_copy(m):
        return pltpu.make_async_copy(x_hbm.at[:, m], y_ref.at[m], xsem.at[m])

    for m in range(members):
        x_copy(m).start()

    def r_copy(u, src):
        return pltpu.make_async_remote_copy(src, rin.at[u], rsend.at[u], rrecv.at[u], device_id={"lev": d + 1}, device_id_type=MESH)

    def q_copy(u, src):
        return pltpu.make_async_remote_copy(src, qin.at[u], qsend.at[u], qrecv.at[u], device_id={"lev": d - 1}, device_id_type=MESH)

    def left_copy(m):
        return pltpu.make_async_remote_copy(hs.at[m, 0], hin.at[m, 1], hsend.at[m, 0], hrecv.at[m, 1], device_id={"col": c - 1}, device_id_type=MESH)

    def right_copy(m):
        return pltpu.make_async_remote_copy(hs.at[m, 1], hin.at[m, 0], hsend.at[m, 1], hrecv.at[m, 0], device_id={"col": c + 1}, device_id_type=MESH)

    def kleft_copy():
        return pltpu.make_async_remote_copy(ks.at[0], kin.at[1], ksend.at[0], krecv.at[1], device_id={"col": c - 1}, device_id_type=MESH)

    def kright_copy():
        return pltpu.make_async_remote_copy(ks.at[1], kin.at[0], ksend.at[1], krecv.at[0], device_id={"col": c + 1}, device_id_type=MESH)

    @pl.when(d == 0)
    def _():
        rin[...] = jnp.zeros_like(rin)

    @pl.when(d == n_lev - 1)
    def _():
        qin[...] = jnp.zeros_like(qin)

    @pl.when(c == 0)
    def _():
        kin[0] = jnp.zeros(kin.shape[1:], jnp.float32)
        hin[:, 0] = jnp.zeros((members,) + hin.shape[2:], jnp.float32)

    @pl.when(c == n_col - 1)
    def _():
        kin[1] = jnp.zeros(kin.shape[1:], jnp.float32)
        hin[:, 1] = jnp.zeros((members,) + hin.shape[2:], jnp.float32)

    ks[...] = jnp.zeros_like(ks)
    ks[0, 0:SMOOTH] = kap_ref[0:SMOOTH]
    ks[1, 0:SMOOTH] = kap_ref[lons - SMOOTH : lons]

    w_copy.wait()
    state = jnp.ones((lons, lats), jnp.float32)
    for k in range(levels):
        bv[k] = 1.0 - wv[k]
        state = state * wv[k]
        G[0, k] = state
    C[0] = state
    state = jnp.ones((lons, lats), jnp.float32)
    for k in reversed(range(levels)):
        state = state * wv[k]
        G[3, k] = state

    def forward(src, dst):
        state = jnp.zeros((lons, lats), jnp.float32)
        for k in range(levels):
            state = wv[k] * state + bv[k] * G[src, k]
            G[dst, k] = state
        return state

    def backward(src, dst):
        state = jnp.zeros((lons, lats), jnp.float32)
        for k in reversed(range(levels)):
            state = wv[k] * state + bv[k] * G[src, k]
            G[dst, k] = state
        return state

    C[1] = backward(0, 2)
    C[2] = forward(3, 1)
    C[3] = forward(2, 0)
    C[4] = backward(0, 0)
    C[5] = backward(1, 1)
    p, cc, a, e, g, h = (C.at[i] for i in range(6))

    pl.semaphore_wait(barrier, sum(there.astype(jnp.int32) for there in (has_low, has_high, has_left, has_right)))

    @pl.when(d == 0)
    def _():
        rout[0, 0] = a[...]
        rout[0, 1] = a[...]
        r_copy(0, rout.at[0]).start()

    @pl.when(d == n_lev - 1)
    def _():
        qout[0, 0] = cc[...]
        qout[0, 1] = g[...]
        q_copy(0, qout.at[0]).start()

    @pl.when(has_left)
    def _():
        kleft_copy().start()

    @pl.when(has_right)
    def _():
        kright_copy().start()

    @pl.loop(0, members // PAIR)
    def _(i):
        first = i * PAIR
        for j in range(PAIR):
            x_copy(first + j).wait()
        for order, slot in ((range(levels), 0), (range(levels - 1, -1, -1), 2), (range(levels), 1), (range(levels - 1, -1, -1), 3)):
            states = [jnp.zeros((lons, lats), jnp.float32)] * PAIR
            for k in order:
                weight, rest = wv[k], bv[k]
                for j in range(PAIR):
                    states[j] = weight * states[j] + rest * y_ref[first + j, k]
                    y_ref[first + j, k] = states[j]
            for j in range(PAIR):
                E[first + j, slot] = states[j]

        @pl.when(d == 0)
        def _():
            for j in range(PAIR):
                r_copy(first + j + 1, E.at[first + j, pl.ds(0, 2)]).start()

        @pl.when(d == n_lev - 1)
        def _():
            for j in range(PAIR):
                q_copy(first + j + 1, E.at[first + j, pl.ds(2, 2)]).start()

    @pl.when(has_left)
    def _():
        kright = pltpu.make_async_remote_copy(ks.at[1], kin.at[0], ksend.at[1], krecv.at[0], device_id={"col": c - 1}, device_id_type=MESH)
        kright.wait_recv()

    @pl.when(has_right)
    def _():
        kleft = pltpu.make_async_remote_copy(ks.at[0], kin.at[1], ksend.at[0], krecv.at[1], device_id={"col": c + 1}, device_id_type=MESH)
        kleft.wait_recv()

    kw[...] = jnp.zeros_like(kw)
    kw[8 - SMOOTH : 8] = kin[0, 0:SMOOTH]
    kw[8 : 8 + lons] = kap_ref[...]
    kw[8 + lons : 8 + lons + SMOOTH] = kin[1, 0:SMOOTH]
    kappa = kw[...]
    lane = lax.broadcasted_iota(jnp.int32, kappa.shape, 1)
    kc[0] = 1.0 - 4.0 * kappa
    kc[1] = jnp.where(lane > 0, kappa, 0.0)
    kc[2] = jnp.where(lane < lats - 1, kappa, 0.0)

    def r_wait(u):
        r_copy(u, rout.at[u]).wait_recv()

    def q_wait(u):
        q_copy(u, qout.at[u]).wait_recv()

    def r_forward(u):
        r_wait(u)

        @pl.when(u == 0)
        def _():
            rho = a[...] + p[...] * p[...] * rin[0, 0]
            rout[0, 0] = rho
            rout[0, 1] = rho

        @pl.when(u > 0)
        def _():
            m = u - 1
            f1_in, f2_in = rin[u, 0], rin[u, 1]
            b1_out = E[m, 2] + cc[...] * f1_in
            f2_in = f2_in + rin[0, 0] * b1_out
            rout[u, 0] = E[m, 0] + p[...] * f1_in
            rout[u, 1] = E[m, 1] + p[...] * f2_in + e[...] * f1_in

        r_copy(u, rout.at[u]).start()

    def q_forward(u):
        q_wait(u)

        @pl.when(u == 0)
        def _():
            k1, k2 = qin[0, 0], qin[0, 1]
            qout[0, 0] = cc[...] + p[...] * p[...] * k1
            qout[0, 1] = g[...] + p[...] * (h[...] * k1 + p[...] * k2 + k1 * (e[...] + a[...] * p[...] * k1))

        @pl.when(u > 0)
        def _():
            m = u - 1
            k1, k2 = qin[0, 0], qin[0, 1]
            f1 = E[m, 0]
            b1_in = qin[u, 0] + k1 * f1
            f2 = E[m, 1] + a[...] * b1_in
            b2_in = qin[u, 1] + k2 * f1 + k1 * f2
            qout[u, 0] = E[m, 2] + p[...] * b1_in
            qout[u, 1] = E[m, 3] + p[...] * b2_in + h[...] * b1_in

        q_copy(u, qout.at[u]).start()

    def finish(m):
        u = m + 1
        for t in range(lons // 8):
            rows = pl.ds(8 * t, 8)
            rho, k1, k2 = rin[0, 0, rows], qin[0, 0, rows], qin[0, 1, rows]
            pp, c1, aa, ee = p[rows], cc[rows], a[rows], e[rows]
            f1_in = rin[u, 0, rows]
            f1 = E[m, 0, rows] + pp * f1_in
            b1_in = qin[u, 0, rows] + k1 * f1
            b1 = E[m, 2, rows] + c1 * f1_in + pp * b1_in
            f2_in = rin[u, 1, rows] + rho * b1
            f2 = E[m, 1, rows] + pp * f2_in + ee * f1_in + aa * b1_in
            b2_in = qin[u, 1, rows] + k2 * f1 + k1 * f2
            for k in range(levels):
                value = y_ref[m, k, rows] + (G[0, k, rows] * f1_in + G[1, k, rows] * b1_in) + (G[2, k, rows] * f2_in + G[3, k, rows] * b2_in)
                U[m, k, 8 + 8 * t : 16 + 8 * t] = value
                if t == 0:
                    hs[m, 0, SMOOTH * k : SMOOTH * (k + 1)] = value[0:SMOOTH]
                if t == lons // 8 - 1:
                    hs[m, 1, SMOOTH * k : SMOOTH * (k + 1)] = value[8 - SMOOTH : 8]

        @pl.when(has_left)
        def _():
            left_copy(m).start()

        @pl.when(has_right)
        def _():
            right_copy(m).start()

    def diffuse(m):
        @pl.when(has_left)
        def _():
            pltpu.make_async_remote_copy(hs.at[m, 1], hin.at[m, 0], hsend.at[m, 1], hrecv.at[m, 0], device_id={"col": c - 1}, device_id_type=MESH).wait_recv()

        @pl.when(has_right)
        def _():
            pltpu.make_async_remote_copy(hs.at[m, 0], hin.at[m, 1], hsend.at[m, 0], hrecv.at[m, 1], device_id={"col": c + 1}, device_id_type=MESH).wait_recv()

        for k in range(levels):
            U[m, k, 8 - SMOOTH : 8] = hin[m, 0, SMOOTH * k : SMOOTH * (k + 1)]
            U[m, k, 8 + lons : 8 + lons + SMOOTH] = hin[m, 1, SMOOTH * k : SMOOTH * (k + 1)]
        for s in range(SMOOTH):
            src = U.at[m] if s % 2 == 0 else T
            dst = T if s % 2 == 0 else U.at[m]
            last = s == SMOOTH - 1
            start = 8 - SMOOTH + 1 + s
            tiles = lons // 8 + (0 if last else 1)
            for t in range(tiles):
                row = start + 8 * t
                keep, north, south, both = kc[0, row : row + 8], kc[1, row : row + 8], kc[2, row : row + 8], kw[row : row + 8]
                for k in range(levels):
                    center = src[k, row : row + 8]
                    value = keep * center + both * (src[k, row - 1 : row + 7] + src[k, row + 1 : row + 9])
                    value = value + (north * pltpu.roll(center, 1, 1) + south * pltpu.roll(center, lats - 1, 1))
                    if last:
                        y_ref[m, k, row - 8 : row] = value
                    else:
                        dst[k, row : row + 8] = value

    units = members + 1

    @pl.loop(0, units + LAG + HALO_LAG)
    def _(step):
        @pl.when(step < units)
        def _():
            @pl.when(jnp.logical_and(middle, d == 1))
            def _():
                r_forward(step)

            @pl.when(jnp.logical_and(middle, d == 2))
            def _():
                q_forward(step)

        unit = step - LAG

        @pl.when(jnp.logical_and(unit >= 0, unit < units))
        def _():
            @pl.when(d == 0)
            def _():
                q_wait(unit)

            @pl.when(d == n_lev - 1)
            def _():
                r_wait(unit)

            @pl.when(jnp.logical_and(middle, d == 1))
            def _():
                q_forward(unit)

            @pl.when(jnp.logical_and(middle, d == 2))
            def _():
                r_forward(unit)

            @pl.when(unit > 0)
            def _():
                finish(unit - 1)

        done = step - LAG - HALO_LAG - 1

        @pl.when(done >= 0)
        def _():
            diffuse(done)

    @pl.loop(0, units)
    def _(u):
        @pl.when(has_high)
        def _():
            r_copy(u, rout.at[u]).wait_send()

        @pl.when(has_low)
        def _():
            q_copy(u, qout.at[u]).wait_send()

    @pl.loop(0, members)
    def _(m):
        @pl.when(has_left)
        def _():
            left_copy(m).wait_send()

        @pl.when(has_right)
        def _():
            right_copy(m).wait_send()

    @pl.when(has_left)
    def _():
        kleft_copy().wait_send()

    @pl.when(has_right)
    def _():
        kright_copy().wait_send()


def write_kernel(y_ref, out_hbm, sems):
    members = y_ref.shape[0]
    copies = [pltpu.make_async_copy(y_ref.at[m], out_hbm.at[:, m], sems.at[m]) for m in range(members)]
    for copy in copies:
        copy.start()
    for copy in copies:
        copy.wait()


def solution(mesh):
    n_lev, n_col = mesh.shape["lev"], mesh.shape["col"]

    def per_device(control_field, decay_rate, diffusivity):
        levels, members, lons, lats = control_field.shape
        units = members + 1
        f32 = jnp.float32
        vmem = lambda *shape: pltpu.VMEM(shape, f32)
        dma = lambda *shape: pltpu.SemaphoreType.DMA(shape)
        state = (lons, lats)
        halo = (SMOOTH * levels, lats)
        y = pl.pallas_call(
            functools.partial(kernel, n_lev, n_col),
            out_shape=pltpu.VMEM((members, levels, lons, lats), f32),
            in_specs=[pl.BlockSpec(memory_space=pltpu.HBM), pl.BlockSpec(memory_space=pltpu.HBM), pl.BlockSpec(memory_space=pltpu.VMEM)],
            out_specs=pl.BlockSpec(memory_space=pltpu.VMEM),
            scratch_shapes=[
                vmem(levels, *state), vmem(levels, *state), vmem(4, levels, *state), vmem(6, *state), vmem(members, 4, *state),
                vmem(units, 2, *state), vmem(units, 2, *state), vmem(units, 2, *state), vmem(units, 2, *state),
                vmem(members, 2, *halo), vmem(members, 2, *halo),
                vmem(members, levels, lons + 16, lats), vmem(levels, lons + 16, lats),
                vmem(2, 8, lats), vmem(2, 8, lats), vmem(lons + 16, lats), vmem(3, lons + 16, lats),
                dma(), dma(members), dma(units), dma(units), dma(units), dma(units),
                dma(members, 2), dma(members, 2), dma(2), dma(2),
            ],
            compiler_params=pltpu.CompilerParams(collective_id=0, has_side_effects=True, vmem_limit_bytes=48 * 2**20),
        )(control_field, decay_rate, diffusivity)
        return pl.pallas_call(
            write_kernel,
            out_shape=jax.ShapeDtypeStruct(control_field.shape, f32),
            in_specs=[pl.BlockSpec(memory_space=pltpu.VMEM)],
            out_specs=pl.BlockSpec(memory_space=pl.ANY),
            scratch_shapes=[dma(members)],
            compiler_params=pltpu.CompilerParams(vmem_limit_bytes=8 * 2**20),
        )(y)

    in_specs = (P("lev", None, "col", None), P("lev", "col", None), P("col", None))
    return jax.shard_map(per_device, mesh=mesh, in_specs=in_specs, out_specs=P("lev", None, "col", None), check_vma=False)
```

```python
import functools

import jax
import jax.numpy as jnp
from jax import lax
from jax.experimental import pallas as pl
from jax.experimental.pallas import tpu as pltpu
from jax.sharding import PartitionSpec as P

MESH = pl.DeviceIdType.MESH
SMOOTH = 4
PAIR = 2
LAG = 6
HALO_LAG = 6


def diffuse(fields, put_last, ksh, tri, TT, levels, lons, lats):
    for s in range(SMOOTH):
        last = s == SMOOTH - 1
        for t in range(lons // 8 + (0 if last else 1)):
            for q in range(PAIR):
                src = fields[q] if s == 0 else TT[s - 1].at[q]
                first = (8 - SMOOTH if s == 0 else 0) + 8 * t
                both = ksh[s, 8 * t : 8 * t + 8]
                west, mid, east = (pl.ds(first + j, 8) for j in range(3))

                def put(k, value):
                    if last:
                        put_last(q, k, t, value)
                    else:
                        TT[s][q, k, 8 * t : 8 * t + 8] = value

                if q % 2:
                    lane = lax.broadcasted_iota(jnp.int32, both.shape, 1)
                    keep, north, south = 1.0 - 4.0 * both, jnp.where(lane > 0, both, 0.0), jnp.where(lane < lats - 1, both, 0.0)
                    for k in range(levels):
                        center = src[k, mid]
                        sides = north * pltpu.roll(center, 1, 1) + south * pltpu.roll(center, lats - 1, 1)
                        put(k, keep * center + both * (src[k, west] + src[k, east]) + sides)
                else:
                    center = src[:, mid].reshape(levels * 8, lats)
                    high = center.astype(jnp.bfloat16)
                    low = (center - high.astype(jnp.float32)).astype(jnp.bfloat16)
                    sides = jnp.dot(jnp.concatenate([high, low], axis=1), tri[...], preferred_element_type=jnp.float32)
                    sides = sides.reshape(levels, 8, lats)
                    for k in range(levels):
                        put(k, src[k, mid] + both * ((src[k, west] + src[k, east]) + sides[k]))


def second_difference(tri, lats):
    away = jnp.abs(lax.broadcasted_iota(jnp.int32, tri.shape, 0) % lats - lax.broadcasted_iota(jnp.int32, tri.shape, 1))
    tri[...] = jnp.where(away == 0, -4.0, jnp.where(away == 1, 1.0, 0.0)).astype(jnp.bfloat16)


def kernel(n_lev, n_col, x_hbm, w_hbm, kap_hbm, y_ref, U, ksh, kap_ref, wv, bv, G, C, E, rin, rout, qin, qout, hs, hin, TT, ks, kin, kw,
           tri, wsem, kapsem, xsem, rsend, rrecv, qsend, qrecv, hsend, hrecv, ksend, krecv):
    levels, members, lons, lats = x_hbm.shape
    d, c = lax.axis_index("lev"), lax.axis_index("col")
    has_low, has_high = d > 0, d < n_lev - 1
    has_left, has_right = c > 0, c < n_col - 1
    middle = jnp.logical_and(has_low, has_high)

    barrier = pltpu.get_barrier_semaphore()
    for there, where in ((has_low, {"lev": d - 1}), (has_high, {"lev": d + 1}), (has_left, {"col": c - 1}), (has_right, {"col": c + 1})):
        @pl.when(there)
        def _():
            pl.semaphore_signal(barrier, inc=1, device_id=where, device_id_type=MESH)

    w_copy = pltpu.make_async_copy(w_hbm, wv, wsem)
    w_copy.start()
    kap_copy = pltpu.make_async_copy(kap_hbm, kap_ref, kapsem)
    kap_copy.start()

    def x_copy(m):
        return pltpu.make_async_copy(x_hbm.at[:, m], y_ref.at[m], xsem.at[m])

    for m in range(members):
        x_copy(m).start()

    def r_copy(u, src):
        return pltpu.make_async_remote_copy(src, rin.at[u], rsend.at[u], rrecv.at[u], device_id={"lev": d + 1}, device_id_type=MESH)

    def q_copy(u, src):
        return pltpu.make_async_remote_copy(src, qin.at[u], qsend.at[u], qrecv.at[u], device_id={"lev": d - 1}, device_id_type=MESH)

    def left_copy(m):
        return pltpu.make_async_remote_copy(hs.at[m, 0], hin.at[m, 1], hsend.at[m, 0], hrecv.at[m, 1], device_id={"col": c - 1}, device_id_type=MESH)

    def right_copy(m):
        return pltpu.make_async_remote_copy(hs.at[m, 1], hin.at[m, 0], hsend.at[m, 1], hrecv.at[m, 0], device_id={"col": c + 1}, device_id_type=MESH)

    def kleft_copy():
        return pltpu.make_async_remote_copy(ks.at[0], kin.at[1], ksend.at[0], krecv.at[1], device_id={"col": c - 1}, device_id_type=MESH)

    def kright_copy():
        return pltpu.make_async_remote_copy(ks.at[1], kin.at[0], ksend.at[1], krecv.at[0], device_id={"col": c + 1}, device_id_type=MESH)

    @pl.when(d == 0)
    def _():
        rin[...] = jnp.zeros_like(rin)

    @pl.when(d == n_lev - 1)
    def _():
        qin[...] = jnp.zeros_like(qin)

    @pl.when(c == 0)
    def _():
        kin[0] = jnp.zeros(kin.shape[1:], jnp.float32)
        hin[:, 0] = jnp.zeros((members,) + hin.shape[2:], jnp.float32)

    @pl.when(c == n_col - 1)
    def _():
        kin[1] = jnp.zeros(kin.shape[1:], jnp.float32)
        hin[:, 1] = jnp.zeros((members,) + hin.shape[2:], jnp.float32)

    kap_copy.wait()
    ks[...] = jnp.zeros_like(ks)
    ks[0, 0:SMOOTH] = kap_ref[0:SMOOTH]
    ks[1, 0:SMOOTH] = kap_ref[lons - SMOOTH : lons]

    w_copy.wait()
    state = jnp.ones((lons, lats), jnp.float32)
    for k in range(levels):
        bv[k] = 1.0 - wv[k]
        state = state * wv[k]
        G[0, k] = state
    C[0] = state
    state = jnp.ones((lons, lats), jnp.float32)
    for k in reversed(range(levels)):
        state = state * wv[k]
        G[3, k] = state

    def forward(src, dst):
        state = jnp.zeros((lons, lats), jnp.float32)
        for k in range(levels):
            state = wv[k] * state + bv[k] * G[src, k]
            G[dst, k] = state
        return state

    def backward(src, dst):
        state = jnp.zeros((lons, lats), jnp.float32)
        for k in reversed(range(levels)):
            state = wv[k] * state + bv[k] * G[src, k]
            G[dst, k] = state
        return state

    C[1] = backward(0, 2)
    C[2] = forward(3, 1)
    C[3] = forward(2, 0)
    C[4] = backward(0, 0)
    C[5] = backward(1, 1)
    p, cc, a, e, g, h = (C.at[i] for i in range(6))

    pl.semaphore_wait(barrier, sum(there.astype(jnp.int32) for there in (has_low, has_high, has_left, has_right)))

    @pl.when(d == 0)
    def _():
        rout[0, 0] = a[...]
        rout[0, 1] = a[...]
        r_copy(0, rout.at[0]).start()

    @pl.when(d == n_lev - 1)
    def _():
        qout[0, 0] = cc[...]
        qout[0, 1] = g[...]
        q_copy(0, qout.at[0]).start()

    @pl.when(has_left)
    def _():
        kleft_copy().start()

    @pl.when(has_right)
    def _():
        kright_copy().start()

    @pl.loop(0, members // PAIR)
    def _(i):
        first = i * PAIR
        for j in range(PAIR):
            x_copy(first + j).wait()
        for order, slot in ((range(levels), 0), (range(levels - 1, -1, -1), 2), (range(levels), 1), (range(levels - 1, -1, -1), 3)):
            states = [jnp.zeros((lons, lats), jnp.float32)] * PAIR
            for k in order:
                weight, rest = wv[k], bv[k]
                for j in range(PAIR):
                    states[j] = weight * states[j] + rest * y_ref[first + j, k]
                    y_ref[first + j, k] = states[j]
            for j in range(PAIR):
                E[first + j, slot] = states[j]

        @pl.when(d == 0)
        def _():
            for j in range(PAIR):
                r_copy(first + j + 1, E.at[first + j, pl.ds(0, 2)]).start()

        @pl.when(d == n_lev - 1)
        def _():
            for j in range(PAIR):
                q_copy(first + j + 1, E.at[first + j, pl.ds(2, 2)]).start()

    @pl.when(has_left)
    def _():
        kright = pltpu.make_async_remote_copy(ks.at[1], kin.at[0], ksend.at[1], krecv.at[0], device_id={"col": c - 1}, device_id_type=MESH)
        kright.wait_recv()

    @pl.when(has_right)
    def _():
        kleft = pltpu.make_async_remote_copy(ks.at[0], kin.at[1], ksend.at[0], krecv.at[1], device_id={"col": c + 1}, device_id_type=MESH)
        kleft.wait_recv()

    kw[...] = jnp.zeros_like(kw)
    kw[8 - SMOOTH : 8] = kin[0, 0:SMOOTH]
    kw[8 : 8 + lons] = kap_ref[...]
    kw[8 + lons : 8 + lons + SMOOTH] = kin[1, 0:SMOOTH]
    for s in range(SMOOTH):
        ksh[s] = kw[8 - SMOOTH + 1 + s : 8 - SMOOTH + 1 + s + lons + 8]
    second_difference(tri, lats)

    def r_wait(u):
        r_copy(u, rout.at[u]).wait_recv()

    def q_wait(u):
        q_copy(u, qout.at[u]).wait_recv()

    def r_forward(u):
        r_wait(u)

        @pl.when(u == 0)
        def _():
            rho = a[...] + p[...] * p[...] * rin[0, 0]
            rout[0, 0] = rho
            rout[0, 1] = rho

        @pl.when(u > 0)
        def _():
            m = u - 1
            f1_in, f2_in = rin[u, 0], rin[u, 1]
            b1_out = E[m, 2] + cc[...] * f1_in
            f2_in = f2_in + rin[0, 0] * b1_out
            rout[u, 0] = E[m, 0] + p[...] * f1_in
            rout[u, 1] = E[m, 1] + p[...] * f2_in + e[...] * f1_in

        r_copy(u, rout.at[u]).start()

    def q_forward(u):
        q_wait(u)

        @pl.when(u == 0)
        def _():
            k1, k2 = qin[0, 0], qin[0, 1]
            qout[0, 0] = cc[...] + p[...] * p[...] * k1
            qout[0, 1] = g[...] + p[...] * (h[...] * k1 + p[...] * k2 + k1 * (e[...] + a[...] * p[...] * k1))

        @pl.when(u > 0)
        def _():
            m = u - 1
            k1, k2 = qin[0, 0], qin[0, 1]
            f1 = E[m, 0]
            b1_in = qin[u, 0] + k1 * f1
            f2 = E[m, 1] + a[...] * b1_in
            b2_in = qin[u, 1] + k2 * f1 + k1 * f2
            qout[u, 0] = E[m, 2] + p[...] * b1_in
            qout[u, 1] = E[m, 3] + p[...] * b2_in + h[...] * b1_in

        q_copy(u, qout.at[u]).start()

    def finish(m):
        u = m + 1
        for t in range(lons // 8):
            rows = pl.ds(8 * t, 8)
            rho, k1, k2 = rin[0, 0, rows], qin[0, 0, rows], qin[0, 1, rows]
            pp, c1, aa, ee = p[rows], cc[rows], a[rows], e[rows]
            f1_in = rin[u, 0, rows]
            f1 = E[m, 0, rows] + pp * f1_in
            b1_in = qin[u, 0, rows] + k1 * f1
            b1 = E[m, 2, rows] + c1 * f1_in + pp * b1_in
            f2_in = rin[u, 1, rows] + rho * b1
            f2 = E[m, 1, rows] + pp * f2_in + ee * f1_in + aa * b1_in
            b2_in = qin[u, 1, rows] + k2 * f1 + k1 * f2
            for k in range(levels):
                value = y_ref[m, k, rows] + (G[0, k, rows] * f1_in + G[1, k, rows] * b1_in) + (G[2, k, rows] * f2_in + G[3, k, rows] * b2_in)
                U[m, k, 8 + 8 * t : 16 + 8 * t] = value
                if t == 0:
                    hs[m, 0, SMOOTH * k : SMOOTH * (k + 1)] = value[0:SMOOTH]
                if t == lons // 8 - 1:
                    hs[m, 1, SMOOTH * k : SMOOTH * (k + 1)] = value[8 - SMOOTH : 8]

        @pl.when(has_left)
        def _():
            left_copy(m).start()

        @pl.when(has_right)
        def _():
            right_copy(m).start()

    def take_halo(m):
        @pl.when(has_left)
        def _():
            pltpu.make_async_remote_copy(hs.at[m, 1], hin.at[m, 0], hsend.at[m, 1], hrecv.at[m, 0], device_id={"col": c - 1}, device_id_type=MESH).wait_recv()

        @pl.when(has_right)
        def _():
            pltpu.make_async_remote_copy(hs.at[m, 0], hin.at[m, 1], hsend.at[m, 0], hrecv.at[m, 1], device_id={"col": c + 1}, device_id_type=MESH).wait_recv()

        for k in range(levels):
            U[m, k, 8 - SMOOTH : 8] = hin[m, 0, SMOOTH * k : SMOOTH * (k + 1)]
            U[m, k, 8 + lons : 8 + lons + SMOOTH] = hin[m, 1, SMOOTH * k : SMOOTH * (k + 1)]
    units = members + 1

    @pl.loop(0, units + LAG + HALO_LAG)
    def _(step):
        @pl.when(step < units)
        def _():
            @pl.when(jnp.logical_and(middle, d == 1))
            def _():
                r_forward(step)

            @pl.when(jnp.logical_and(middle, d == 2))
            def _():
                q_forward(step)

        unit = step - LAG

        @pl.when(jnp.logical_and(unit >= 0, unit < units))
        def _():
            @pl.when(d == 0)
            def _():
                q_wait(unit)

            @pl.when(d == n_lev - 1)
            def _():
                r_wait(unit)

            @pl.when(jnp.logical_and(middle, d == 1))
            def _():
                q_forward(unit)

            @pl.when(jnp.logical_and(middle, d == 2))
            def _():
                r_forward(unit)

            @pl.when(unit > 0)
            def _():
                finish(unit - 1)

        done = step - LAG - HALO_LAG - 1

        @pl.when(done >= 0)
        def _():
            take_halo(done)

        @pl.when(jnp.logical_and(jnp.logical_and(done >= 0, done < members - PAIR), done % PAIR == PAIR - 1))
        def _():
            m = done - (PAIR - 1)

            def put_last(q, k, t, value):
                y_ref[m + q, k, 8 * t : 8 * t + 8] = value

            diffuse([U.at[m + q] for q in range(PAIR)], put_last, ksh, tri, TT, levels, lons, lats)

    @pl.loop(0, units)
    def _(u):
        @pl.when(has_high)
        def _():
            r_copy(u, rout.at[u]).wait_send()

        @pl.when(has_low)
        def _():
            q_copy(u, qout.at[u]).wait_send()

    @pl.loop(0, members)
    def _(m):
        @pl.when(has_left)
        def _():
            left_copy(m).wait_send()

        @pl.when(has_right)
        def _():
            right_copy(m).wait_send()

    @pl.when(has_left)
    def _():
        kleft_copy().wait_send()

    @pl.when(has_right)
    def _():
        kright_copy().wait_send()


def write_kernel(y_ref, U, ksh, out_hbm, tri, y_last, TT, sems):
    members, levels, lons, lats = y_ref.shape
    early = members - PAIR
    copies = [pltpu.make_async_copy(y_ref.at[m], out_hbm.at[:, m], sems.at[m]) for m in range(early)]
    copies += [pltpu.make_async_copy(y_last.at[q], out_hbm.at[:, early + q], sems.at[early + q]) for q in range(PAIR)]
    for copy in copies[:early]:
        copy.start()
    second_difference(tri, lats)

    def put_last(q, k, t, value):
        y_last[q, k, 8 * t : 8 * t + 8] = value

    diffuse([U.at[early + q] for q in range(PAIR)], put_last, ksh, tri, TT, levels, lons, lats)
    for copy in copies[early:]:
        copy.start()
    for copy in copies:
        copy.wait()


def solution(mesh):
    n_lev, n_col = mesh.shape["lev"], mesh.shape["col"]

    def per_device(control_field, decay_rate, diffusivity):
        levels, members, lons, lats = control_field.shape
        units = members + 1
        f32 = jnp.float32
        vmem = lambda *shape: pltpu.VMEM(shape, f32)
        dma = lambda *shape: pltpu.SemaphoreType.DMA(shape)
        state = (lons, lats)
        halo = (SMOOTH * levels, lats)
        steps = [vmem(PAIR, levels, lons + 16, lats)] * (SMOOTH - 1)
        triangle = pltpu.VMEM((2 * lats, lats), jnp.bfloat16)
        in_vmem = pl.BlockSpec(memory_space=pltpu.VMEM)
        y, wide, kappas = pl.pallas_call(
            functools.partial(kernel, n_lev, n_col),
            out_shape=[vmem(members, levels, lons, lats), vmem(members, levels, lons + 16, lats), vmem(SMOOTH, lons + 8, lats)],
            in_specs=[pl.BlockSpec(memory_space=pltpu.HBM), pl.BlockSpec(memory_space=pltpu.HBM), pl.BlockSpec(memory_space=pltpu.HBM)],
            out_specs=[in_vmem] * 3,
            scratch_shapes=[
                vmem(*state), vmem(levels, *state), vmem(levels, *state), vmem(4, levels, *state), vmem(6, *state), vmem(members, 4, *state),
                vmem(units, 2, *state), vmem(units, 2, *state), vmem(units, 2, *state), vmem(units, 2, *state),
                vmem(members, 2, *halo), vmem(members, 2, *halo),
                steps,
                vmem(2, 8, lats), vmem(2, 8, lats), vmem(lons + 16, lats), triangle,
                dma(), dma(), dma(members), dma(units), dma(units), dma(units), dma(units),
                dma(members, 2), dma(members, 2), dma(2), dma(2),
            ],
            compiler_params=pltpu.CompilerParams(collective_id=0, has_side_effects=True, vmem_limit_bytes=32 * 2**20),
        )(*(pltpu.with_memory_space_constraint(x, pltpu.HBM) for x in (control_field, decay_rate, diffusivity)))
        return pl.pallas_call(
            write_kernel,
            out_shape=jax.ShapeDtypeStruct(control_field.shape, f32),
            in_specs=[in_vmem] * 3,
            out_specs=pl.BlockSpec(memory_space=pl.ANY),
            scratch_shapes=[triangle, vmem(PAIR, levels, lons, lats), steps, dma(members)],
            compiler_params=pltpu.CompilerParams(vmem_limit_bytes=12 * 2**20),
        )(y, wide, kappas)

    in_specs = (P("lev", None, "col", None), P("lev", "col", None), P("col", None))
    return jax.shard_map(per_device, mesh=mesh, in_specs=in_specs, out_specs=P("lev", None, "col", None), check_vma=False)
```

```python
import functools

import jax
import jax.numpy as jnp
from jax import lax
from jax.experimental import pallas as pl
from jax.experimental.pallas import tpu as pltpu
from jax.sharding import PartitionSpec as P

MESH = pl.DeviceIdType.MESH
SMOOTH = 4
PAIR = 2
LAG = 6
HALO_LAG = 7
LATER = 6


def diffuse(fields, put_last, ksh, tri, TT, levels, lons, lats):
    for s in range(SMOOTH):
        last = s == SMOOTH - 1
        for t in range(lons // 8 + (0 if last else 1)):
            for q in range(PAIR):
                src = fields[q] if s == 0 else TT[s - 1].at[q]
                first = (8 - SMOOTH if s == 0 else 0) + 8 * t
                both = ksh[s, 8 * t : 8 * t + 8]
                west, mid, east = (pl.ds(first + j, 8) for j in range(3))

                def put(k, value):
                    if last:
                        put_last(q, k, t, value)
                    else:
                        TT[s][q, k, 8 * t : 8 * t + 8] = value

                keep = 1.0 - 4.0 * both
                if q % 2:
                    lane = lax.broadcasted_iota(jnp.int32, both.shape, 1)
                    north, south = jnp.where(lane > 0, both, 0.0), jnp.where(lane < lats - 1, both, 0.0)
                    for k in range(levels):
                        center = src[k, mid]
                        sides = north * pltpu.roll(center, 1, 1) + south * pltpu.roll(center, lats - 1, 1)
                        put(k, keep * center + both * (src[k, west] + src[k, east]) + sides)
                else:
                    center = src[:, mid].reshape(levels * 8, lats)
                    high = center.astype(jnp.bfloat16)
                    low = (center - high.astype(jnp.float32)).astype(jnp.bfloat16)
                    sides = jnp.dot(jnp.concatenate([high, low], axis=1), tri[...], preferred_element_type=jnp.float32)
                    sides = sides.reshape(levels, 8, lats)
                    for k in range(levels):
                        put(k, keep * src[k, mid] + both * ((src[k, west] + src[k, east]) + sides[k]))


def neighbours(tri, lats):
    away = jnp.abs(lax.broadcasted_iota(jnp.int32, tri.shape, 0) % lats - lax.broadcasted_iota(jnp.int32, tri.shape, 1))
    tri[...] = jnp.where(away == 1, 1.0, 0.0).astype(jnp.bfloat16)


def kernel(n_lev, n_col, x_hbm, w_hbm, kap_hbm, y_ref, U, ksh, kap_ref, wv, bv, G, C, E, rin, rout, qin, qout, hs, hin, TT, ks, kin, kw,
           tri, wsem, kapsem, xsem, rsend, rrecv, qsend, qrecv, hsend, hrecv, ksend, krecv):
    levels, members, lons, lats = x_hbm.shape
    d, c = lax.axis_index("lev"), lax.axis_index("col")
    has_low, has_high = d > 0, d < n_lev - 1
    has_left, has_right = c > 0, c < n_col - 1
    middle = jnp.logical_and(has_low, has_high)

    barrier = pltpu.get_barrier_semaphore()
    for there, where in ((has_low, {"lev": d - 1}), (has_high, {"lev": d + 1}), (has_left, {"col": c - 1}), (has_right, {"col": c + 1})):
        @pl.when(there)
        def _():
            pl.semaphore_signal(barrier, inc=1, device_id=where, device_id_type=MESH)

    w_copy = pltpu.make_async_copy(w_hbm, wv, wsem)
    w_copy.start()
    kap_copy = pltpu.make_async_copy(kap_hbm, kap_ref, kapsem)
    kap_copy.start()

    def x_copy(m):
        return pltpu.make_async_copy(x_hbm.at[:, m], y_ref.at[m], xsem.at[m])

    for m in range(PAIR):
        x_copy(m).start()

    def r_copy(u, src):
        return pltpu.make_async_remote_copy(src, rin.at[u], rsend.at[u], rrecv.at[u], device_id={"lev": d + 1}, device_id_type=MESH)

    def q_copy(u, src):
        return pltpu.make_async_remote_copy(src, qin.at[u], qsend.at[u], qrecv.at[u], device_id={"lev": d - 1}, device_id_type=MESH)

    def left_copy(m):
        return pltpu.make_async_remote_copy(hs.at[m, 0], hin.at[m, 1], hsend.at[m, 0], hrecv.at[m, 1], device_id={"col": c - 1}, device_id_type=MESH)

    def right_copy(m):
        return pltpu.make_async_remote_copy(hs.at[m, 1], hin.at[m, 0], hsend.at[m, 1], hrecv.at[m, 0], device_id={"col": c + 1}, device_id_type=MESH)

    def kleft_copy():
        return pltpu.make_async_remote_copy(ks.at[0], kin.at[1], ksend.at[0], krecv.at[1], device_id={"col": c - 1}, device_id_type=MESH)

    def kright_copy():
        return pltpu.make_async_remote_copy(ks.at[1], kin.at[0], ksend.at[1], krecv.at[0], device_id={"col": c + 1}, device_id_type=MESH)

    @pl.when(d == 0)
    def _():
        rin[...] = jnp.zeros_like(rin)

    @pl.when(d == n_lev - 1)
    def _():
        qin[...] = jnp.zeros_like(qin)

    @pl.when(c == 0)
    def _():
        kin[0] = jnp.zeros(kin.shape[1:], jnp.float32)
        hin[:, 0] = jnp.zeros((members,) + hin.shape[2:], jnp.float32)

    @pl.when(c == n_col - 1)
    def _():
        kin[1] = jnp.zeros(kin.shape[1:], jnp.float32)
        hin[:, 1] = jnp.zeros((members,) + hin.shape[2:], jnp.float32)

    kap_copy.wait()
    ks[...] = jnp.zeros_like(ks)
    ks[0, 0:SMOOTH] = kap_ref[0:SMOOTH]
    ks[1, 0:SMOOTH] = kap_ref[lons - SMOOTH : lons]

    w_copy.wait()
    for m in range(PAIR, members):
        x_copy(m).start()
    state = jnp.ones((lons, lats), jnp.float32)
    for k in range(levels):
        bv[k] = 1.0 - wv[k]
        state = state * wv[k]
        G[0, k] = state
    C[0] = state
    state = jnp.ones((lons, lats), jnp.float32)
    for k in reversed(range(levels)):
        state = state * wv[k]
        G[3, k] = state

    def forward(src, dst):
        state = jnp.zeros((lons, lats), jnp.float32)
        for k in range(levels):
            state = wv[k] * state + bv[k] * G[src, k]
            G[dst, k] = state
        return state

    def backward(src, dst):
        state = jnp.zeros((lons, lats), jnp.float32)
        for k in reversed(range(levels)):
            state = wv[k] * state + bv[k] * G[src, k]
            G[dst, k] = state
        return state

    C[1] = backward(0, 2)
    C[2] = forward(3, 1)
    C[3] = forward(2, 0)
    C[4] = backward(0, 0)
    C[5] = backward(1, 1)
    p, cc, a, e, g, h = (C.at[i] for i in range(6))

    pl.semaphore_wait(barrier, sum(there.astype(jnp.int32) for there in (has_low, has_high, has_left, has_right)))

    @pl.when(d == 0)
    def _():
        rout[0, 0] = a[...]
        rout[0, 1] = a[...]
        r_copy(0, rout.at[0]).start()

    @pl.when(d == n_lev - 1)
    def _():
        qout[0, 0] = cc[...]
        qout[0, 1] = g[...]
        q_copy(0, qout.at[0]).start()

    @pl.when(has_left)
    def _():
        kleft_copy().start()

    @pl.when(has_right)
    def _():
        kright_copy().start()

    @pl.loop(0, members // PAIR)
    def _(i):
        first = i * PAIR
        for j in range(PAIR):
            x_copy(first + j).wait()
        for order, slot in ((range(levels), 0), (range(levels - 1, -1, -1), 2), (range(levels), 1), (range(levels - 1, -1, -1), 3)):
            states = [jnp.zeros((lons, lats), jnp.float32)] * PAIR
            for k in order:
                weight, rest = wv[k], bv[k]
                for j in range(PAIR):
                    states[j] = weight * states[j] + rest * y_ref[first + j, k]
                    y_ref[first + j, k] = states[j]
            for j in range(PAIR):
                E[first + j, slot] = states[j]

        @pl.when(d == 0)
        def _():
            for j in range(PAIR):
                r_copy(first + j + 1, E.at[first + j, pl.ds(0, 2)]).start()

        @pl.when(d == n_lev - 1)
        def _():
            for j in range(PAIR):
                q_copy(first + j + 1, E.at[first + j, pl.ds(2, 2)]).start()

    @pl.when(has_left)
    def _():
        kright = pltpu.make_async_remote_copy(ks.at[1], kin.at[0], ksend.at[1], krecv.at[0], device_id={"col": c - 1}, device_id_type=MESH)
        kright.wait_recv()

    @pl.when(has_right)
    def _():
        kleft = pltpu.make_async_remote_copy(ks.at[0], kin.at[1], ksend.at[0], krecv.at[1], device_id={"col": c + 1}, device_id_type=MESH)
        kleft.wait_recv()

    kw[...] = jnp.zeros_like(kw)
    kw[8 - SMOOTH : 8] = kin[0, 0:SMOOTH]
    kw[8 : 8 + lons] = kap_ref[...]
    kw[8 + lons : 8 + lons + SMOOTH] = kin[1, 0:SMOOTH]
    for s in range(SMOOTH):
        ksh[s] = kw[8 - SMOOTH + 1 + s : 8 - SMOOTH + 1 + s + lons + 8]
    neighbours(tri, lats)

    def r_wait(u):
        r_copy(u, rout.at[u]).wait_recv()

    def q_wait(u):
        q_copy(u, qout.at[u]).wait_recv()

    def r_forward(u):
        r_wait(u)

        @pl.when(u == 0)
        def _():
            rho = a[...] + p[...] * p[...] * rin[0, 0]
            rout[0, 0] = rho
            rout[0, 1] = rho

        @pl.when(u > 0)
        def _():
            m = u - 1
            f1_in, f2_in = rin[u, 0], rin[u, 1]
            b1_out = E[m, 2] + cc[...] * f1_in
            f2_in = f2_in + rin[0, 0] * b1_out
            rout[u, 0] = E[m, 0] + p[...] * f1_in
            rout[u, 1] = E[m, 1] + p[...] * f2_in + e[...] * f1_in

        r_copy(u, rout.at[u]).start()

    def q_forward(u):
        q_wait(u)

        @pl.when(u == 0)
        def _():
            k1, k2 = qin[0, 0], qin[0, 1]
            qout[0, 0] = cc[...] + p[...] * p[...] * k1
            qout[0, 1] = g[...] + p[...] * (h[...] * k1 + p[...] * k2 + k1 * (e[...] + a[...] * p[...] * k1))

        @pl.when(u > 0)
        def _():
            m = u - 1
            k1, k2 = qin[0, 0], qin[0, 1]
            f1 = E[m, 0]
            b1_in = qin[u, 0] + k1 * f1
            f2 = E[m, 1] + a[...] * b1_in
            b2_in = qin[u, 1] + k2 * f1 + k1 * f2
            qout[u, 0] = E[m, 2] + p[...] * b1_in
            qout[u, 1] = E[m, 3] + p[...] * b2_in + h[...] * b1_in

        q_copy(u, qout.at[u]).start()

    def finish(m):
        u = m + 1
        for t in range(lons // 8):
            rows = pl.ds(8 * t, 8)
            rho, k1, k2 = rin[0, 0, rows], qin[0, 0, rows], qin[0, 1, rows]
            pp, c1, aa, ee = p[rows], cc[rows], a[rows], e[rows]
            f1_in = rin[u, 0, rows]
            f1 = E[m, 0, rows] + pp * f1_in
            b1_in = qin[u, 0, rows] + k1 * f1
            b1 = E[m, 2, rows] + c1 * f1_in + pp * b1_in
            f2_in = rin[u, 1, rows] + rho * b1
            f2 = E[m, 1, rows] + pp * f2_in + ee * f1_in + aa * b1_in
            b2_in = qin[u, 1, rows] + k2 * f1 + k1 * f2
            for k in range(levels):
                value = y_ref[m, k, rows] + (G[0, k, rows] * f1_in + G[1, k, rows] * b1_in) + (G[2, k, rows] * f2_in + G[3, k, rows] * b2_in)
                U[m, k, 8 + 8 * t : 16 + 8 * t] = value
                if t == 0:
                    hs[m, 0, SMOOTH * k : SMOOTH * (k + 1)] = value[0:SMOOTH]
                if t == lons // 8 - 1:
                    hs[m, 1, SMOOTH * k : SMOOTH * (k + 1)] = value[8 - SMOOTH : 8]

        @pl.when(has_left)
        def _():
            left_copy(m).start()

        @pl.when(has_right)
        def _():
            right_copy(m).start()

    def take_halo(m):
        @pl.when(has_left)
        def _():
            pltpu.make_async_remote_copy(hs.at[m, 1], hin.at[m, 0], hsend.at[m, 1], hrecv.at[m, 0], device_id={"col": c - 1}, device_id_type=MESH).wait_recv()

        @pl.when(has_right)
        def _():
            pltpu.make_async_remote_copy(hs.at[m, 0], hin.at[m, 1], hsend.at[m, 0], hrecv.at[m, 1], device_id={"col": c + 1}, device_id_type=MESH).wait_recv()

        for k in range(levels):
            U[m, k, 8 - SMOOTH : 8] = hin[m, 0, SMOOTH * k : SMOOTH * (k + 1)]
            U[m, k, 8 + lons : 8 + lons + SMOOTH] = hin[m, 1, SMOOTH * k : SMOOTH * (k + 1)]
    units = members + 1

    @pl.loop(0, units + LAG + HALO_LAG + LATER)
    def _(step):
        @pl.when(step < units)
        def _():
            @pl.when(jnp.logical_and(middle, d == 1))
            def _():
                r_forward(step)

            @pl.when(jnp.logical_and(middle, d == 2))
            def _():
                q_forward(step)

        unit = step - LAG

        @pl.when(jnp.logical_and(unit >= 0, unit < units))
        def _():
            @pl.when(d == 0)
            def _():
                q_wait(unit)

            @pl.when(d == n_lev - 1)
            def _():
                r_wait(unit)

            @pl.when(jnp.logical_and(middle, d == 1))
            def _():
                q_forward(unit)

            @pl.when(jnp.logical_and(middle, d == 2))
            def _():
                r_forward(unit)

            @pl.when(unit > 0)
            def _():
                finish(unit - 1)

        done = step - LAG - HALO_LAG - 1 - jnp.where(middle, LATER, 0)

        @pl.when(jnp.logical_and(done >= 0, done < members))
        def _():
            take_halo(done)

        @pl.when(jnp.logical_and(jnp.logical_and(done >= 0, done < members - PAIR), done % PAIR == PAIR - 1))
        def _():
            m = done - (PAIR - 1)

            def put_last(q, k, t, value):
                y_ref[m + q, k, 8 * t : 8 * t + 8] = value

            diffuse([U.at[m + q] for q in range(PAIR)], put_last, ksh, tri, TT, levels, lons, lats)

    @pl.loop(0, units)
    def _(u):
        @pl.when(has_high)
        def _():
            r_copy(u, rout.at[u]).wait_send()

        @pl.when(has_low)
        def _():
            q_copy(u, qout.at[u]).wait_send()

    @pl.loop(0, members)
    def _(m):
        @pl.when(has_left)
        def _():
            left_copy(m).wait_send()

        @pl.when(has_right)
        def _():
            right_copy(m).wait_send()

    @pl.when(has_left)
    def _():
        kleft_copy().wait_send()

    @pl.when(has_right)
    def _():
        kright_copy().wait_send()


def write_kernel(y_ref, U, ksh, out_hbm, tri, y_last, TT, sems):
    members, levels, lons, lats = y_ref.shape
    early = members - PAIR
    copies = [pltpu.make_async_copy(y_ref.at[m], out_hbm.at[:, m], sems.at[m]) for m in range(early)]
    copies += [pltpu.make_async_copy(y_last.at[q], out_hbm.at[:, early + q], sems.at[early + q]) for q in range(PAIR)]
    for copy in copies[:early]:
        copy.start()
    neighbours(tri, lats)

    def put_last(q, k, t, value):
        y_last[q, k, 8 * t : 8 * t + 8] = value

    diffuse([U.at[early + q] for q in range(PAIR)], put_last, ksh, tri, TT, levels, lons, lats)
    for copy in copies[early:]:
        copy.start()
    for copy in copies:
        copy.wait()


def solution(mesh):
    n_lev, n_col = mesh.shape["lev"], mesh.shape["col"]

    def per_device(control_field, decay_rate, diffusivity):
        levels, members, lons, lats = control_field.shape
        units = members + 1
        f32 = jnp.float32
        vmem = lambda *shape: pltpu.VMEM(shape, f32)
        dma = lambda *shape: pltpu.SemaphoreType.DMA(shape)
        state = (lons, lats)
        halo = (SMOOTH * levels, lats)
        steps = [vmem(PAIR, levels, lons + 16, lats)] * (SMOOTH - 1)
        triangle = pltpu.VMEM((2 * lats, lats), jnp.bfloat16)
        in_vmem = pl.BlockSpec(memory_space=pltpu.VMEM)
        y, wide, kappas = pl.pallas_call(
            functools.partial(kernel, n_lev, n_col),
            out_shape=[vmem(members, levels, lons, lats), vmem(members, levels, lons + 16, lats), vmem(SMOOTH, lons + 8, lats)],
            in_specs=[pl.BlockSpec(memory_space=pltpu.HBM), pl.BlockSpec(memory_space=pltpu.HBM), pl.BlockSpec(memory_space=pltpu.HBM)],
            out_specs=[in_vmem] * 3,
            scratch_shapes=[
                vmem(*state), vmem(levels, *state), vmem(levels, *state), vmem(4, levels, *state), vmem(6, *state), vmem(members, 4, *state),
                vmem(units, 2, *state), vmem(units, 2, *state), vmem(units, 2, *state), vmem(units, 2, *state),
                vmem(members, 2, *halo), vmem(members, 2, *halo),
                steps,
                vmem(2, 8, lats), vmem(2, 8, lats), vmem(lons + 16, lats), triangle,
                dma(), dma(), dma(members), dma(units), dma(units), dma(units), dma(units),
                dma(members, 2), dma(members, 2), dma(2), dma(2),
            ],
            compiler_params=pltpu.CompilerParams(collective_id=0, has_side_effects=True, vmem_limit_bytes=32 * 2**20),
        )(*(pltpu.with_memory_space_constraint(x, pltpu.HBM) for x in (control_field, decay_rate, diffusivity)))
        return pl.pallas_call(
            write_kernel,
            out_shape=jax.ShapeDtypeStruct(control_field.shape, f32),
            in_specs=[in_vmem] * 3,
            out_specs=pl.BlockSpec(memory_space=pl.ANY),
            scratch_shapes=[triangle, vmem(PAIR, levels, lons, lats), steps, dma(members)],
            compiler_params=pltpu.CompilerParams(vmem_limit_bytes=12 * 2**20),
        )(y, wide, kappas)

    in_specs = (P("lev", None, "col", None), P("lev", "col", None), P("col", None))
    return jax.shard_map(per_device, mesh=mesh, in_specs=in_specs, out_specs=P("lev", None, "col", None), check_vma=False)
```

```python
import functools

import jax
import jax.numpy as jnp
from jax import lax
from jax.experimental import pallas as pl
from jax.experimental.pallas import tpu as pltpu
from jax.sharding import PartitionSpec as P

MESH = pl.DeviceIdType.MESH
SMOOTH = 4
PAIR = 2
LAG = 6
HALO_LAG = 7
LATER = 6


def diffuse(fields, put_last, ksh, tri, TT, levels, lons, lats):
    for s in range(SMOOTH):
        last = s == SMOOTH - 1
        for t in range(lons // 8 + (0 if last else 1)):
            for q in range(PAIR):
                src = fields[q] if s == 0 else TT[s - 1].at[q]
                first = (8 - SMOOTH if s == 0 else 0) + 8 * t
                both = ksh[s, 8 * t : 8 * t + 8]
                west, mid, east = (pl.ds(first + j, 8) for j in range(3))

                def put(k, value):
                    if last:
                        put_last(q, k, t, value)
                    else:
                        TT[s][q, k, 8 * t : 8 * t + 8] = value

                keep = 1.0 - 4.0 * both
                if (q + t) % 2:
                    lane = lax.broadcasted_iota(jnp.int32, both.shape, 1)
                    north, south = jnp.where(lane > 0, both, 0.0), jnp.where(lane < lats - 1, both, 0.0)
                    for k in range(levels):
                        center = src[k, mid]
                        sides = north * pltpu.roll(center, 1, 1) + south * pltpu.roll(center, lats - 1, 1)
                        put(k, keep * center + both * (src[k, west] + src[k, east]) + sides)
                else:
                    center = src[:, mid].reshape(levels * 8, lats)
                    high = center.astype(jnp.bfloat16)
                    low = (center - high.astype(jnp.float32)).astype(jnp.bfloat16)
                    sides = jnp.dot(jnp.concatenate([high, low], axis=1), tri[...], preferred_element_type=jnp.float32)
                    sides = sides.reshape(levels, 8, lats)
                    for k in range(levels):
                        put(k, keep * src[k, mid] + both * ((src[k, west] + src[k, east]) + sides[k]))


def neighbours(tri, lats):
    away = jnp.abs(lax.broadcasted_iota(jnp.int32, tri.shape, 0) % lats - lax.broadcasted_iota(jnp.int32, tri.shape, 1))
    tri[...] = jnp.where(away == 1, 1.0, 0.0).astype(jnp.bfloat16)


def kernel(n_lev, n_col, x_hbm, w_hbm, kap_hbm, y_ref, U, ksh, kap_ref, wv, bv, G, C, E, rin, rout, qin, qout, hs, hin, TT, ks, kin, kw,
           tri, wsem, kapsem, xsem, rsend, rrecv, qsend, qrecv, hsend, hrecv, ksend, krecv):
    levels, members, lons, lats = x_hbm.shape
    d, c = lax.axis_index("lev"), lax.axis_index("col")
    has_low, has_high = d > 0, d < n_lev - 1
    has_left, has_right = c > 0, c < n_col - 1
    middle = jnp.logical_and(has_low, has_high)

    barrier = pltpu.get_barrier_semaphore()
    for there, where in ((has_low, {"lev": d - 1}), (has_high, {"lev": d + 1}), (has_left, {"col": c - 1}), (has_right, {"col": c + 1})):
        @pl.when(there)
        def _():
            pl.semaphore_signal(barrier, inc=1, device_id=where, device_id_type=MESH)

    w_copy = pltpu.make_async_copy(w_hbm, wv, wsem)
    w_copy.start()
    kap_copy = pltpu.make_async_copy(kap_hbm, kap_ref, kapsem)
    kap_copy.start()

    def x_copy(m):
        return pltpu.make_async_copy(x_hbm.at[:, m], y_ref.at[m], xsem.at[m])

    for m in range(PAIR):
        x_copy(m).start()

    def r_copy(u, src):
        return pltpu.make_async_remote_copy(src, rin.at[u], rsend.at[u], rrecv.at[u], device_id={"lev": d + 1}, device_id_type=MESH)

    def q_copy(u, src):
        return pltpu.make_async_remote_copy(src, qin.at[u], qsend.at[u], qrecv.at[u], device_id={"lev": d - 1}, device_id_type=MESH)

    def left_copy(m):
        return pltpu.make_async_remote_copy(hs.at[m, 0], hin.at[m, 1], hsend.at[m, 0], hrecv.at[m, 1], device_id={"col": c - 1}, device_id_type=MESH)

    def right_copy(m):
        return pltpu.make_async_remote_copy(hs.at[m, 1], hin.at[m, 0], hsend.at[m, 1], hrecv.at[m, 0], device_id={"col": c + 1}, device_id_type=MESH)

    def kleft_copy():
        return pltpu.make_async_remote_copy(ks.at[0], kin.at[1], ksend.at[0], krecv.at[1], device_id={"col": c - 1}, device_id_type=MESH)

    def kright_copy():
        return pltpu.make_async_remote_copy(ks.at[1], kin.at[0], ksend.at[1], krecv.at[0], device_id={"col": c + 1}, device_id_type=MESH)

    @pl.when(d == 0)
    def _():
        rin[...] = jnp.zeros_like(rin)

    @pl.when(d == n_lev - 1)
    def _():
        qin[...] = jnp.zeros_like(qin)

    @pl.when(c == 0)
    def _():
        kin[0] = jnp.zeros(kin.shape[1:], jnp.float32)
        hin[:, 0] = jnp.zeros((members,) + hin.shape[2:], jnp.float32)

    @pl.when(c == n_col - 1)
    def _():
        kin[1] = jnp.zeros(kin.shape[1:], jnp.float32)
        hin[:, 1] = jnp.zeros((members,) + hin.shape[2:], jnp.float32)

    kap_copy.wait()
    ks[...] = jnp.zeros_like(ks)
    ks[0, 0:SMOOTH] = kap_ref[0:SMOOTH]
    ks[1, 0:SMOOTH] = kap_ref[lons - SMOOTH : lons]

    w_copy.wait()
    for m in range(PAIR, members):
        x_copy(m).start()
    state = jnp.ones((lons, lats), jnp.float32)
    for k in range(levels):
        bv[k] = 1.0 - wv[k]
        state = state * wv[k]
        G[0, k] = state
    C[0] = state
    state = jnp.ones((lons, lats), jnp.float32)
    for k in reversed(range(levels)):
        state = state * wv[k]
        G[3, k] = state

    def forward(src, dst):
        state = jnp.zeros((lons, lats), jnp.float32)
        for k in range(levels):
            state = wv[k] * state + bv[k] * G[src, k]
            G[dst, k] = state
        return state

    def backward(src, dst):
        state = jnp.zeros((lons, lats), jnp.float32)
        for k in reversed(range(levels)):
            state = wv[k] * state + bv[k] * G[src, k]
            G[dst, k] = state
        return state

    C[1] = backward(0, 2)
    C[2] = forward(3, 1)
    C[3] = forward(2, 0)
    C[4] = backward(0, 0)
    C[5] = backward(1, 1)
    p, cc, a, e, g, h = (C.at[i] for i in range(6))

    pl.semaphore_wait(barrier, sum(there.astype(jnp.int32) for there in (has_low, has_high, has_left, has_right)))

    @pl.when(d == 0)
    def _():
        rout[0, 0] = a[...]
        rout[0, 1] = a[...]
        r_copy(0, rout.at[0]).start()

    @pl.when(d == n_lev - 1)
    def _():
        qout[0, 0] = cc[...]
        qout[0, 1] = g[...]
        q_copy(0, qout.at[0]).start()

    @pl.when(has_left)
    def _():
        kleft_copy().start()

    @pl.when(has_right)
    def _():
        kright_copy().start()

    @pl.loop(0, members // PAIR)
    def _(i):
        first = i * PAIR
        for j in range(PAIR):
            x_copy(first + j).wait()
        for order, slot in ((range(levels), 0), (range(levels - 1, -1, -1), 2), (range(levels), 1), (range(levels - 1, -1, -1), 3)):
            states = [jnp.zeros((lons, lats), jnp.float32)] * PAIR
            for k in order:
                weight, rest = wv[k], bv[k]
                for j in range(PAIR):
                    states[j] = weight * states[j] + rest * y_ref[first + j, k]
                    y_ref[first + j, k] = states[j]
            for j in range(PAIR):
                E[first + j, slot] = states[j]

        @pl.when(d == 0)
        def _():
            for j in range(PAIR):
                r_copy(first + j + 1, E.at[first + j, pl.ds(0, 2)]).start()

        @pl.when(d == n_lev - 1)
        def _():
            for j in range(PAIR):
                q_copy(first + j + 1, E.at[first + j, pl.ds(2, 2)]).start()

    @pl.when(has_left)
    def _():
        kright = pltpu.make_async_remote_copy(ks.at[1], kin.at[0], ksend.at[1], krecv.at[0], device_id={"col": c - 1}, device_id_type=MESH)
        kright.wait_recv()

    @pl.when(has_right)
    def _():
        kleft = pltpu.make_async_remote_copy(ks.at[0], kin.at[1], ksend.at[0], krecv.at[1], device_id={"col": c + 1}, device_id_type=MESH)
        kleft.wait_recv()

    kw[...] = jnp.zeros_like(kw)
    kw[8 - SMOOTH : 8] = kin[0, 0:SMOOTH]
    kw[8 : 8 + lons] = kap_ref[...]
    kw[8 + lons : 8 + lons + SMOOTH] = kin[1, 0:SMOOTH]
    for s in range(SMOOTH):
        ksh[s] = kw[8 - SMOOTH + 1 + s : 8 - SMOOTH + 1 + s + lons + 8]
    neighbours(tri, lats)

    def r_wait(u):
        r_copy(u, rout.at[u]).wait_recv()

    def q_wait(u):
        q_copy(u, qout.at[u]).wait_recv()

    def r_forward(u):
        r_wait(u)

        @pl.when(u == 0)
        def _():
            rho = a[...] + p[...] * p[...] * rin[0, 0]
            rout[0, 0] = rho
            rout[0, 1] = rho

        @pl.when(u > 0)
        def _():
            m = u - 1
            f1_in, f2_in = rin[u, 0], rin[u, 1]
            b1_out = E[m, 2] + cc[...] * f1_in
            f2_in = f2_in + rin[0, 0] * b1_out
            rout[u, 0] = E[m, 0] + p[...] * f1_in
            rout[u, 1] = E[m, 1] + p[...] * f2_in + e[...] * f1_in

        r_copy(u, rout.at[u]).start()

    def q_forward(u):
        q_wait(u)

        @pl.when(u == 0)
        def _():
            k1, k2 = qin[0, 0], qin[0, 1]
            qout[0, 0] = cc[...] + p[...] * p[...] * k1
            qout[0, 1] = g[...] + p[...] * (h[...] * k1 + p[...] * k2 + k1 * (e[...] + a[...] * p[...] * k1))

        @pl.when(u > 0)
        def _():
            m = u - 1
            k1, k2 = qin[0, 0], qin[0, 1]
            f1 = E[m, 0]
            b1_in = qin[u, 0] + k1 * f1
            f2 = E[m, 1] + a[...] * b1_in
            b2_in = qin[u, 1] + k2 * f1 + k1 * f2
            qout[u, 0] = E[m, 2] + p[...] * b1_in
            qout[u, 1] = E[m, 3] + p[...] * b2_in + h[...] * b1_in

        q_copy(u, qout.at[u]).start()

    def finish(m):
        u = m + 1
        for t in range(lons // 8):
            rows = pl.ds(8 * t, 8)
            rho, k1, k2 = rin[0, 0, rows], qin[0, 0, rows], qin[0, 1, rows]
            pp, c1, aa, ee = p[rows], cc[rows], a[rows], e[rows]
            f1_in = rin[u, 0, rows]
            f1 = E[m, 0, rows] + pp * f1_in
            b1_in = qin[u, 0, rows] + k1 * f1
            b1 = E[m, 2, rows] + c1 * f1_in + pp * b1_in
            f2_in = rin[u, 1, rows] + rho * b1
            f2 = E[m, 1, rows] + pp * f2_in + ee * f1_in + aa * b1_in
            b2_in = qin[u, 1, rows] + k2 * f1 + k1 * f2
            for k in range(levels):
                value = y_ref[m, k, rows] + (G[0, k, rows] * f1_in + G[1, k, rows] * b1_in) + (G[2, k, rows] * f2_in + G[3, k, rows] * b2_in)
                U[m, k, 8 + 8 * t : 16 + 8 * t] = value
                if t == 0:
                    hs[m, 0, SMOOTH * k : SMOOTH * (k + 1)] = value[0:SMOOTH]
                if t == lons // 8 - 1:
                    hs[m, 1, SMOOTH * k : SMOOTH * (k + 1)] = value[8 - SMOOTH : 8]

        @pl.when(has_left)
        def _():
            left_copy(m).start()

        @pl.when(has_right)
        def _():
            right_copy(m).start()

    def take_halo(m):
        @pl.when(has_left)
        def _():
            pltpu.make_async_remote_copy(hs.at[m, 1], hin.at[m, 0], hsend.at[m, 1], hrecv.at[m, 0], device_id={"col": c - 1}, device_id_type=MESH).wait_recv()

        @pl.when(has_right)
        def _():
            pltpu.make_async_remote_copy(hs.at[m, 0], hin.at[m, 1], hsend.at[m, 0], hrecv.at[m, 1], device_id={"col": c + 1}, device_id_type=MESH).wait_recv()

        for k in range(levels):
            U[m, k, 8 - SMOOTH : 8] = hin[m, 0, SMOOTH * k : SMOOTH * (k + 1)]
            U[m, k, 8 + lons : 8 + lons + SMOOTH] = hin[m, 1, SMOOTH * k : SMOOTH * (k + 1)]
    units = members + 1

    @pl.loop(0, units + LAG + HALO_LAG + LATER)
    def _(step):
        @pl.when(step < units)
        def _():
            @pl.when(jnp.logical_and(middle, d == 1))
            def _():
                r_forward(step)

            @pl.when(jnp.logical_and(middle, d == 2))
            def _():
                q_forward(step)

        unit = step - LAG

        @pl.when(jnp.logical_and(unit >= 0, unit < units))
        def _():
            @pl.when(d == 0)
            def _():
                q_wait(unit)

            @pl.when(d == n_lev - 1)
            def _():
                r_wait(unit)

            @pl.when(jnp.logical_and(middle, d == 1))
            def _():
                q_forward(unit)

            @pl.when(jnp.logical_and(middle, d == 2))
            def _():
                r_forward(unit)

            @pl.when(unit > 0)
            def _():
                finish(unit - 1)

        done = step - LAG - HALO_LAG - 1 - jnp.where(middle, LATER, 0)

        @pl.when(jnp.logical_and(done >= 0, done < members))
        def _():
            take_halo(done)

        @pl.when(jnp.logical_and(jnp.logical_and(done >= 0, done < members - PAIR), done % PAIR == PAIR - 1))
        def _():
            m = done - (PAIR - 1)

            def put_last(q, k, t, value):
                y_ref[m + q, k, 8 * t : 8 * t + 8] = value

            diffuse([U.at[m + q] for q in range(PAIR)], put_last, ksh, tri, TT, levels, lons, lats)

    @pl.loop(0, units)
    def _(u):
        @pl.when(has_high)
        def _():
            r_copy(u, rout.at[u]).wait_send()

        @pl.when(has_low)
        def _():
            q_copy(u, qout.at[u]).wait_send()

    @pl.loop(0, members)
    def _(m):
        @pl.when(has_left)
        def _():
            left_copy(m).wait_send()

        @pl.when(has_right)
        def _():
            right_copy(m).wait_send()

    @pl.when(has_left)
    def _():
        kleft_copy().wait_send()

    @pl.when(has_right)
    def _():
        kright_copy().wait_send()


def write_kernel(y_ref, U, ksh, out_hbm, tri, y_last, TT, sems):
    members, levels, lons, lats = y_ref.shape
    early = members - PAIR
    copies = [pltpu.make_async_copy(y_ref.at[m], out_hbm.at[:, m], sems.at[m]) for m in range(early)]
    copies += [pltpu.make_async_copy(y_last.at[q], out_hbm.at[:, early + q], sems.at[early + q]) for q in range(PAIR)]
    for copy in copies[:early]:
        copy.start()
    neighbours(tri, lats)

    def put_last(q, k, t, value):
        y_last[q, k, 8 * t : 8 * t + 8] = value

    diffuse([U.at[early + q] for q in range(PAIR)], put_last, ksh, tri, TT, levels, lons, lats)
    for copy in copies[early:]:
        copy.start()
    for copy in copies:
        copy.wait()


def solution(mesh):
    n_lev, n_col = mesh.shape["lev"], mesh.shape["col"]

    def per_device(control_field, decay_rate, diffusivity):
        levels, members, lons, lats = control_field.shape
        units = members + 1
        f32 = jnp.float32
        vmem = lambda *shape: pltpu.VMEM(shape, f32)
        dma = lambda *shape: pltpu.SemaphoreType.DMA(shape)
        state = (lons, lats)
        halo = (SMOOTH * levels, lats)
        steps = [vmem(PAIR, levels, lons + 16, lats)] * (SMOOTH - 1)
        triangle = pltpu.VMEM((2 * lats, lats), jnp.bfloat16)
        in_vmem = pl.BlockSpec(memory_space=pltpu.VMEM)
        y, wide, kappas = pl.pallas_call(
            functools.partial(kernel, n_lev, n_col),
            out_shape=[vmem(members, levels, lons, lats), vmem(members, levels, lons + 16, lats), vmem(SMOOTH, lons + 8, lats)],
            in_specs=[pl.BlockSpec(memory_space=pltpu.HBM), pl.BlockSpec(memory_space=pltpu.HBM), pl.BlockSpec(memory_space=pltpu.HBM)],
            out_specs=[in_vmem] * 3,
            scratch_shapes=[
                vmem(*state), vmem(levels, *state), vmem(levels, *state), vmem(4, levels, *state), vmem(6, *state), vmem(members, 4, *state),
                vmem(units, 2, *state), vmem(units, 2, *state), vmem(units, 2, *state), vmem(units, 2, *state),
                vmem(members, 2, *halo), vmem(members, 2, *halo),
                steps,
                vmem(2, 8, lats), vmem(2, 8, lats), vmem(lons + 16, lats), triangle,
                dma(), dma(), dma(members), dma(units), dma(units), dma(units), dma(units),
                dma(members, 2), dma(members, 2), dma(2), dma(2),
            ],
            compiler_params=pltpu.CompilerParams(collective_id=0, has_side_effects=True, vmem_limit_bytes=32 * 2**20),
        )(*(pltpu.with_memory_space_constraint(x, pltpu.HBM) for x in (control_field, decay_rate, diffusivity)))
        return pl.pallas_call(
            write_kernel,
            out_shape=jax.ShapeDtypeStruct(control_field.shape, f32),
            in_specs=[in_vmem] * 3,
            out_specs=pl.BlockSpec(memory_space=pl.ANY),
            scratch_shapes=[triangle, vmem(PAIR, levels, lons, lats), steps, dma(members)],
            compiler_params=pltpu.CompilerParams(vmem_limit_bytes=12 * 2**20),
        )(y, wide, kappas)

    in_specs = (P("lev", None, "col", None), P("lev", "col", None), P("col", None))
    return jax.shard_map(per_device, mesh=mesh, in_specs=in_specs, out_specs=P("lev", None, "col", None), check_vma=False)
```
